128 devices in a mesh: tok: 8 (over x_lo, z), feat: 16 (over y, x_hi, core).
Axes of the slice: x: 4 (x_hi: 2, x_lo: 2; x = x_hi * 2 + x_lo), y: 4, z: 4, core: 2. Of those that a mesh axis runs over, the one named last changes fastest.
Arguments:
- activations: float32 [2048, 8192], P('tok', 'feat'), may hold values from -40 to 40
- gradients: float32 [2048, 28672], P('tok', 'feat'), may hold values from -40 to 40
- input_basis: float32 [8192, 8192], P('feat', 'tok'), may hold values from -0.09375 to 0.09375
- output_basis: float32 [28672, 1792], P('feat', 'tok'), may hold values from -0.046875 to 0.046875
Outputs:
- eigenvalues: float32 [8192, 1792], P('tok', 'feat')
The draws below stay inside these ranges and needn't reach their ends.
All inputs are finite; a program needn't handle non-finite values.
Results may differ from the reference program's by a relative error of at most 0.00016.
Values sent between devices are 32-bit elements; how exact they have to be, the bound alone decides.
No kernel may reach another device: no remote copies, remote signals or barrier semaphores. Data moves between devices by JAX's collectives and lax.ppermute only.
A program may use at most 128 MiB of HBM per device.

```python
import jax
import jax.numpy as jnp
from jax import lax

D = 8192
DOUT = 28672
WINDOW = 1792
TOKENS = 2048


def token_matrix(key, count, width):
    noise = jnp.clip(jax.random.normal(jax.random.fold_in(key, 11), (count, width), jnp.float32), -6.0, 6.0)
    ramp = 1.0 + 2.0 * jnp.arange(count, dtype=jnp.float32) / (count - 1)
    rough = jnp.exp(jax.random.uniform(jax.random.fold_in(key, 14), (count,), jnp.float32, -0.35, 0.35))
    factor = 0.6 * ramp * rough
    return noise * factor[:, None]


def draw_activations(key, part):
    return token_matrix(jax.random.fold_in(key, 101), TOKENS, D)


def draw_gradients(key, part):
    return token_matrix(jax.random.fold_in(key, 202), TOKENS, DOUT)


def with_spikes(values, key, source, target, parts, factor):
    def block_of(position):
        return (jnp.arange(values.shape[position]) // (values.shape[position] // parts)).reshape((-1,) + (1,) * (values.ndim - 1 - position))

    first = jax.random.permutation(key, parts)[block_of(target)]
    other_side = (block_of(target) + parts // 2) % parts
    return jnp.where((block_of(source) == first) | (block_of(source) == other_side), factor * values, values)


def level_of(rng, dims, split, least, top_value):
    loudness, own = 1.0, jax.random.fold_in(rng, 6)
    for axis_at, blocks in split:
        steps = jnp.exp(jax.random.uniform(jax.random.fold_in(own, axis_at), (blocks,), jnp.float32, least / len(split), top_value / len(split)))
        loudness = loudness * jnp.repeat(steps, dims[axis_at] // blocks).reshape([-1 if axis == axis_at else 1 for axis in range(len(dims))])
    return loudness


def bell_draw_with(own_key, extent, scale, reach, cuts, heavy, held_as=jnp.bfloat16):
    entries = scale * jax.random.normal(own_key, extent, jnp.float32)
    if cuts:
        entries = entries * level_of(own_key, extent, cuts, -0.22, 0.18)
    return jnp.clip(with_spikes(entries, jax.random.fold_in(own_key, 3), *heavy), -reach, reach).astype(held_as)


def setup_inputs(seed: int = 0) -> dict:
    splits = jax.random.split(jax.random.key(seed), 5)
    activations = draw_activations(jax.random.fold_in(splits[4], 71), 0)
    gradients = draw_gradients(jax.random.fold_in(splits[4], 71), 0)
    input_basis = bell_draw_with(splits[2], (D, D), D ** -0.5, 0.09375, ((0, 16), (1, 8)), (0, 1, 16, 2.0), jnp.float32)
    output_basis = bell_draw_with(splits[3], (DOUT, WINDOW), DOUT ** -0.5, 0.046875, ((0, 16), (1, 8)), (0, 1, 16, 2.0), jnp.float32)
    return dict(activations=activations, gradients=gradients, input_basis=input_basis, output_basis=output_basis)


def reference(activations, gradients, input_basis, output_basis):
    highest = lax.Precision.HIGHEST
    input_coords = jnp.dot(activations, input_basis, precision=highest, preferred_element_type=jnp.float32)
    output_coords = jnp.dot(gradients, output_basis, precision=highest, preferred_element_type=jnp.float32)
    input_squares = input_coords * input_coords
    output_squares = output_coords * output_coords
    summed = jnp.dot(input_squares.T, output_squares, precision=highest, preferred_element_type=jnp.float32)
    return summed / TOKENS
```

```python
import jax
import jax.numpy as jnp
from jax import lax
from jax.sharding import PartitionSpec as P

AXES = ("tok", "feat")


def coords(i):
    return i // 64, i // 16 % 4, i // 4 % 4, i // 2 % 2, i % 2


def linear(xl, z, y, xh, c):
    return (((xl % 2) * 4 + z % 4) * 4 + y % 4) * 4 + (xh % 2) * 2 + c % 2


def send(value, target):
    pairs = []
    for i in range(128):
        to = target(*coords(i))
        if to is not None:
            pairs.append((i, linear(*to)))
    return lax.ppermute(value, AXES, pairs)


def z_by(d):
    return lambda xl, z, y, xh, c: (xl, z + d, y, xh, c)


def y_by(d):
    return lambda xl, z, y, xh, c: (xl, z, y + d, xh, c)


def other_xlo(xl, z, y, xh, c):
    return (1 - xl, z, y, xh, c)


def other_xhi(xl, z, y, xh, c):
    return (xl, z, y, 1 - xh, c)


def other_core(xl, z, y, xh, c):
    return (xl, z, y, xh, 1 - c)


def near(xl, z, y, xh, c):
    return (xl, z, y ^ 1, xh, c) if y // 2 == xl else None


def step(xl, z, y, xh, c):
    return (xl, z, 3 - y, xh, c) if y // 2 != xl else None


def jump(xl, z, y, xh, c):
    return (xl, z, y ^ 2, xh, c) if y // 2 != xl else None


def over(xl, z, y, xh, c):
    return (1 - xl, z, y, xh, c) if y // 2 == xl else None


def after(value, *earlier):
    return lax.optimization_barrier((value, *earlier))[0]


def split(x):
    hi = lax.reduce_precision(x, 8, 7)
    return hi.astype(jnp.bfloat16), (x - hi).astype(jnp.bfloat16)


def dot(left, right, dims):
    return lax.dot_general(left, right, (dims, ((), ())), preferred_element_type=jnp.float32)


def dot3(left, right, dims):
    (l_hi, l_lo), (r_hi, r_lo) = left, right
    return dot(l_hi, r_hi, dims) + (dot(l_lo, r_hi, dims) + dot(l_hi, r_lo, dims))


def rows_at(value, index, size):
    return lax.dynamic_slice_in_dim(value, index * size, size, 0)


def chunk(value, index):
    return lax.dynamic_index_in_dim(value, index, 0, keepdims=False)


def per_device(activations, gradients, input_basis, output_basis):
    tok, feat = lax.axis_index("tok"), lax.axis_index("feat")
    z, y = tok % 4, feat // 4
    xh, core = feat // 2 % 2, feat % 2
    xl = tok // 4
    first = core == 0

    a = activations
    ax = send(a, other_xlo)
    a_l, a_r = send(a, z_by(1)), send(a, z_by(-1))
    ax_l, ax_r = send(ax, z_by(1)), send(ax, z_by(-1))
    a_f = send(a_l, z_by(1))
    ax_f = send(ax_r, z_by(-1))

    g = gradients
    gx = send(g, other_xlo)
    bt = output_basis.T
    half = bt.shape[1] // 2
    b0, b1 = bt[:, :half], bt[:, half:]
    b0_l, b0_r = send(b0, z_by(1)), send(b0, z_by(-1))
    b1_l, b1_r = send(b1, z_by(1)), send(b1, z_by(-1))

    width = input_basis.shape[1] // 2
    keep_b = split(lax.dynamic_slice_in_dim(input_basis, core * width, width, 1))
    send_b = split(lax.dynamic_slice_in_dim(input_basis, (1 - core) * width, width, 1))
    rows = lambda p, d, n: rows_at(p, (y + d) % 4, n)
    n = a.shape[0]
    h = n // 2

    def input_group(pieces):
        tokens = split(jnp.concatenate(pieces, 0))
        return dot3(tokens, send_b, ((1,), (0,))), dot3(tokens, keep_b, ((1,), (0,)))

    def first_hop(part):
        far = rows(part, 2, n)
        return far, send(far[:h], y_by(1)), send(far[h:], y_by(-1))

    def second_hop(part, from_l, from_r):
        up, down = rows(part, 1, n), rows(part, 3, n)
        up = jnp.concatenate([up[:h] + from_l, up[h:]], 0)
        down = jnp.concatenate([down[:h], down[h:] + from_r], 0)
        return up, send(up, y_by(1)), send(down, y_by(-1))

    away0, here0 = input_group([a, ax, a_l, ax_l])
    part0 = here0 + send(away0, other_core)
    far0, l0, r0 = first_hop(part0)
    late = [after(p, far0) for p in (a_r, ax_r, a_f, ax_f)]
    away1, here1 = input_group(late)
    from_core1 = send(away1, other_core)
    up0, l20, r20 = second_hop(part0, after(l0, here1), after(r0, here1))
    part1 = here1 + after(from_core1, up0)
    far1, l1, r1 = first_hop(part1)
    b0_f = send(after(b0_l, far1), z_by(1))

    both_g = jnp.concatenate([g, after(gx, up0)], 0)
    g_halves = [split(both_g[:, k * half : (k + 1) * half]) for k in range(2)]
    g_halves = lax.optimization_barrier(g_halves)

    def coords_t(p0, p1, dep):
        p0, p1 = lax.optimization_barrier((split(after(p0, dep)), split(after(p1, dep))))
        return dot3(p0, g_halves[0], ((1,), (1,))) + dot3(p1, g_halves[1], ((1,), (1,)))

    c_own = coords_t(b0, b1, far1)
    mine0 = rows(part0, 0, n) + after(l20, c_own) + after(r20, c_own)
    from_xhi0 = send(mine0, other_xhi)
    up1, l21, r21 = second_hop(part1, after(l1, mine0), after(r1, mine0))
    b1_f = send(after(b1_r, mine0), z_by(-1))
    c_l = coords_t(b0_l, b1_l, up1)
    c_r = coords_t(b0_r, b1_r, up1)

    def square(mine, other):
        both = mine + other
        return both * both

    sq0 = square(mine0, after(from_xhi0, c_r))
    sq0_l, sq0_r = send(sq0, y_by(1)), send(sq0, y_by(-1))
    mine1 = rows(part1, 0, n) + after(l21, sq0) + after(r21, sq0)
    from_xhi1 = send(mine1, other_xhi)
    c_f = coords_t(b0_f, b1_f, mine1)
    c = jnp.stack([c_own, c_r, c_f, c_l])
    o = c.shape[1] // 2
    c0, c1 = c[:, :o], c[:, o:]
    o_away = jnp.where(first, c1, c0)
    u = jnp.where(first, c0, c1) + send(o_away, other_core)
    block_at = lambda zabs: chunk(u, (zabs - z + 8) % 4)
    away = jnp.stack([block_at(1 - xh), block_at(3 - xh)])
    from_xhi = send(away, other_xhi)
    sq0_l, sq0_r = after(sq0_l, away), after(sq0_r, away)
    f0_lo, f0_hi = send(sq0_l[:h], y_by(1)), send(sq0_r[h:], y_by(-1))
    sq1 = square(mine1, after(from_xhi1, sq0_l))
    sq1_l, sq1_r = send(sq1, y_by(1)), send(sq1, y_by(-1))

    v = jnp.stack([block_at(xh), block_at(2 + xh)]) + after(from_xhi, sq1)
    j = y % 2
    crossed, straight = chunk(v, 1 - j), chunk(v, j)
    from_near, from_step = send(crossed, near), send(crossed, step)
    from_jump = send(straight, jump)
    block0 = jnp.concatenate([after(p, crossed) for p in (sq0, sq0_l, sq0_r, f0_lo, f0_hi)], 0)
    other0 = send(block0, other_core)
    sq1_l, sq1_r = after(sq1_l, block0), after(sq1_r, block0)
    f1_lo, f1_hi = send(sq1_l[:h], y_by(1)), send(sq1_r[h:], y_by(-1))

    got = straight + after(from_near, sq1_l) + after(from_step, sq1_l) + after(from_jump, sq1_l)
    sq_o = got * got
    t2 = sq_o.shape[1] // 2
    came = send(sq_o, over)
    block1 = jnp.concatenate([after(p, sq_o) for p in (sq1, sq1_l, sq1_r, f1_lo, f1_hi)], 0)
    other1 = send(block1, other_core)
    came = after(came, block1)
    came = jnp.concatenate([came[:, t2:], came[:, :t2]], 1)
    own_o = jnp.where(y // 2 == xl, sq_o, came)
    o_l, o_r, o_f = send(own_o, z_by(1)), send(own_o, z_by(-1)), send(own_o, z_by(2))
    squares = [[split(after(p, own_o)) for p in pair] for pair in ((block0, other0), (block1, other1))]
    halves = []
    for pair in ((own_o, o_l), (o_r, o_f)):
        chunks = jnp.stack([p[:, k * t2 : (k + 1) * t2] for p in pair for k in range(2)])
        rel = jnp.concatenate([chunk(chunks, (y + d) % 4) for d in (0, 3, 1, 2)], 1)
        hi, lo = split(rel)
        halves.append((jnp.concatenate([hi, lo], 0), hi))

    scale = 1.0 / (8 * activations.shape[0])
    eig = []
    for side in range(2):
        total = 0.0
        for q in range(2):
            s_hi, s_lo = squares[q][side]
            both = dot(halves[q][0], s_hi, ((1,), (0,)))
            total = total + (both[:o] + both[o:] + dot(halves[q][1], s_lo, ((1,), (0,))))
        eig.append(total * scale)
    low = jnp.where(first, eig[0], eig[1])
    high = jnp.where(first, eig[1], eig[0])
    return jnp.concatenate([low, high], 1).T


def solution(mesh):
    in_specs = (P("tok", "feat"), P("tok", "feat"), P("feat", "tok"), P("feat", "tok"))
    out_specs = P("tok", "feat")

    return jax.shard_map(per_device, mesh=mesh, in_specs=in_specs, out_specs=out_specs, check_vma=False)
```

```python
import jax
import jax.numpy as jnp
from jax import lax
from jax.sharding import PartitionSpec as P

AXES = ("tok", "feat")


def coords(i):
    return i // 64, i // 16 % 4, i // 4 % 4, i // 2 % 2, i % 2


def linear(xl, z, y, xh, c):
    return (((xl % 2) * 4 + z % 4) * 4 + y % 4) * 4 + (xh % 2) * 2 + c % 2


def send(value, target):
    pairs = []
    for i in range(128):
        to = target(*coords(i))
        if to is not None:
            pairs.append((i, linear(*to)))
    return lax.ppermute(value, AXES, pairs)


def z_by(d):
    return lambda xl, z, y, xh, c: (xl, z + d, y, xh, c)


def y_by(d):
    return lambda xl, z, y, xh, c: (xl, z, y + d, xh, c)


def other_xlo(xl, z, y, xh, c):
    return (1 - xl, z, y, xh, c)


def other_xhi(xl, z, y, xh, c):
    return (xl, z, y, 1 - xh, c)


def other_core(xl, z, y, xh, c):
    return (xl, z, y, xh, 1 - c)


def near(xl, z, y, xh, c):
    return (xl, z, y ^ 1, xh, c) if y // 2 == xl else None


def step(xl, z, y, xh, c):
    return (xl, z, 3 - y, xh, c) if y // 2 != xl else None


def jump(xl, z, y, xh, c):
    return (xl, z, y ^ 2, xh, c) if y // 2 != xl else None


def over(xl, z, y, xh, c):
    return (1 - xl, z, y, xh, c) if y // 2 == xl else None


def after(value, *earlier):
    return lax.optimization_barrier((value, *earlier))[0]


def split(x):
    hi = lax.reduce_precision(x, 8, 7)
    return hi.astype(jnp.bfloat16), (x - hi).astype(jnp.bfloat16)


def dot(left, right, dims):
    return lax.dot_general(left, right, (dims, ((), ())), preferred_element_type=jnp.float32)


def dot3(left, right, dims):
    (l_hi, l_lo), (r_hi, r_lo) = left, right
    return dot(l_hi, r_hi, dims) + (dot(l_lo, r_hi, dims) + dot(l_hi, r_lo, dims))


def rows_at(value, index, size):
    return lax.dynamic_slice_in_dim(value, index * size, size, 0)


def chunk(value, index):
    return lax.dynamic_index_in_dim(value, index, 0, keepdims=False)


def per_device(activations, gradients, input_basis, output_basis):
    tok, feat = lax.axis_index("tok"), lax.axis_index("feat")
    z, y = tok % 4, feat // 4
    xh, core = feat // 2 % 2, feat % 2
    xl = tok // 4
    first = core == 0

    a = activations
    ax = send(a, other_xlo)
    a_l, a_r = send(a, z_by(1)), send(a, z_by(-1))
    ax_l, ax_r = send(ax, z_by(1)), send(ax, z_by(-1))
    a_f = send(a_l, z_by(1))
    ax_f = send(ax_r, z_by(-1))

    g = gradients
    gx = send(g, other_xlo)
    bt = output_basis.T
    o = bt.shape[0] // 2
    b_l, b_r = send(bt, z_by(1)), send(bt, z_by(-1))

    width = input_basis.shape[1] // 2
    keep_b = split(lax.dynamic_slice_in_dim(input_basis, core * width, width, 1))
    send_b = split(lax.dynamic_slice_in_dim(input_basis, (1 - core) * width, width, 1))
    rows = lambda p, d, n: rows_at(p, (y + d) % 4, n)
    n = a.shape[0]
    h = n // 2

    def input_group(pieces):
        tokens = split(jnp.concatenate(pieces, 0))
        return dot3(tokens, send_b, ((1,), (0,))), dot3(tokens, keep_b, ((1,), (0,)))

    def first_hop(part):
        far = rows(part, 2, n)
        lo, hi = far[:h], far[h:]
        return (lo, hi), send(lo, y_by(1)), send(hi, y_by(-1))

    def second_hop(part, from_l, from_r):
        up, down = rows(part, 1, n), rows(part, 3, n)
        up = jnp.concatenate([up[:h] + from_l, up[h:]], 0)
        down = jnp.concatenate([down[:h], down[h:] + from_r], 0)
        return (up, down), send(up, y_by(1)), send(down, y_by(-1))

    away0, here0 = input_group([after(p, ax_r) for p in (a, ax, a_l, ax_l)])
    part0 = here0 + send(away0, other_core)
    far0, l0, r0 = first_hop(part0)
    away1, here1 = input_group([after(p, *far0) for p in (a_r, ax_r, a_f, ax_f)])
    from_core1 = send(away1, other_core)
    up0, l20, r20 = second_hop(part0, after(l0, here1), after(r0, here1))
    part1 = here1 + after(from_core1, *up0)
    far1, l1, r1 = first_hop(part1)

    b_f0 = send(after(b_l, *far1)[:o], z_by(1))
    mine0 = rows(part0, 0, n) + after(l20, *far1) + after(r20, *far1)
    from_xhi0 = send(mine0, other_xhi)
    up1, l21, r21 = second_hop(part1, after(l1, mine0), after(r1, mine0))
    b_f1 = send(after(b_r, mine0)[o:], z_by(-1))

    both_g = split(jnp.concatenate([g, after(gx, *up1)], 0))
    both_g = lax.optimization_barrier(both_g)

    def coords_t(block, *deps):
        block = lax.optimization_barrier(split(after(block, *deps)))
        return dot3(block, both_g, ((1,), (1,)))

    c_own, c_l = coords_t(bt, *up1), coords_t(b_l, *up1)

    def square(mine, other):
        both = mine + other
        return both * both

    sq0 = square(mine0, after(from_xhi0, c_l))
    sq0_l, sq0_r = send(sq0, y_by(1)), send(sq0, y_by(-1))
    c_r = coords_t(b_r, sq0)
    mine1 = rows(part1, 0, n) + after(l21, c_r) + after(r21, c_r)
    from_xhi1 = send(mine1, other_xhi)
    c_f0, c_f1 = coords_t(b_f0, mine1), coords_t(b_f1, mine1)
    c0 = jnp.stack([c_own[:o], c_r[:o], c_f0, c_l[:o]])
    c1 = jnp.stack([c_own[o:], c_r[o:], c_f1, c_l[o:]])
    o_away = jnp.where(first, c1, c0)
    u = jnp.where(first, c0, c1) + send(o_away, other_core)
    block_at = lambda zabs: chunk(u, (zabs - z + 8) % 4)
    away = jnp.stack([block_at(1 - xh), block_at(3 - xh)])
    from_xhi = send(away, other_xhi)
    sq0_l, sq0_r = after(sq0_l, away), after(sq0_r, away)
    f0_lo, f0_hi = send(sq0_l[:h], y_by(1)), send(sq0_r[h:], y_by(-1))
    sq1 = square(mine1, after(from_xhi1, sq0_l))
    sq1_l, sq1_r = send(sq1, y_by(1)), send(sq1, y_by(-1))

    v = jnp.stack([block_at(xh), block_at(2 + xh)]) + after(from_xhi, sq1)
    j = y % 2
    crossed, straight = chunk(v, 1 - j), chunk(v, j)
    from_near, from_step = send(crossed, near), send(crossed, step)
    from_jump = send(straight, jump)
    got = straight + from_near + from_step + from_jump
    sq_o = got * got
    t2 = sq_o.shape[1] // 2
    came = send(sq_o, over)
    sq1_l, sq1_r = after(sq1_l, sq_o), after(sq1_r, sq_o)
    f1_lo, f1_hi = send(sq1_l[:h], y_by(1)), send(sq1_r[h:], y_by(-1))
    block0 = jnp.concatenate([after(p, sq_o) for p in (sq0, sq0_l, sq0_r, f0_lo, f0_hi)], 0)
    other0 = send(block0, other_core)
    came = after(came, block0, sq1_l)
    came = jnp.concatenate([came[:, t2:], came[:, :t2]], 1)
    own_o = jnp.where(y // 2 == xl, sq_o, came)
    block1 = jnp.concatenate([after(p, own_o) for p in (sq1, sq1_l, sq1_r, f1_lo, f1_hi)], 0)
    other1 = send(block1, other_core)
    o_l, o_r, o_f = send(own_o, z_by(1)), send(own_o, z_by(-1)), send(own_o, z_by(2))
    squares = [[split(after(p, own_o)) for p in pair] for pair in ((block0, other0), (block1, other1))]
    halves = []
    for pair in ((own_o, o_l), (o_r, o_f)):
        chunks = jnp.stack([p[:, k * t2 : (k + 1) * t2] for p in pair for k in range(2)])
        rel = jnp.concatenate([chunk(chunks, (y + d) % 4) for d in (0, 3, 1, 2)], 1)
        hi, lo = split(rel)
        halves.append((jnp.concatenate([hi, lo], 0), hi))

    scale = 1.0 / (8 * activations.shape[0])
    eig = []
    for side in range(2):
        total = 0.0
        for q in range(2):
            s_hi, s_lo = squares[q][side]
            both = dot(halves[q][0], s_hi, ((1,), (0,)))
            total = total + (both[:o] + both[o:] + dot(halves[q][1], s_lo, ((1,), (0,))))
        eig.append(total * scale)
    low = jnp.where(first, eig[0], eig[1])
    high = jnp.where(first, eig[1], eig[0])
    return jnp.concatenate([low, high], 1).T


def solution(mesh):
    in_specs = (P("tok", "feat"), P("tok", "feat"), P("feat", "tok"), P("feat", "tok"))
    out_specs = P("tok", "feat")

    return jax.shard_map(per_device, mesh=mesh, in_specs=in_specs, out_specs=out_specs, check_vma=False)
```
